32 devices in a mesh: row: 4 (over x, core), col: 8 (over z, y).
Axes of the slice: x: 2, y: 2, z: 4, core: 2. Of those that a mesh axis runs over, the one named last changes fastest.
Arguments:
- orbitals: bfloat16 [98304, 4096], P(('row', 'col')), may hold values from -0.09375 to 0.09375
- occupation: int32 [4096], replicated, may hold values from 1 to 128
- owner: int32 [3072, 1], P(('row', 'col')), may hold values from 0 to 7; in each aligned block of 96 rows (0 to 95, 96 to 191, ...) at most 14 rows name the same one
- row_values: bfloat16 [98304, 128], P(('row', 'col')), may hold values from -0.23925781 to 0.23925781
- slab_values: bfloat16 [256, 4096], P(None, ('row', 'col')), may hold values from -6 to 6
- moment_weights: float32 [49, 4096], P(None, ('row', 'col')), may hold values from -0.6 to 0.6
- batch_atom: int32 [32], P(('row', 'col')), may hold values from 0 to 255
- batch_shell: int32 [32], P(('row', 'col')), may hold values from 0 to 63
Outputs:
- density: float32 [4096], P(('row', 'col'))
- moments: float32 [49, 256, 64], P(None, ('row', 'col'))
The draws below stay inside these ranges and needn't reach their ends.
Inputs may be any that keep to these rules, and one draw needn't show every extreme that they name: Among the 96 blocks of one device no owner is named more than 14 times.
All inputs are finite; a program needn't handle non-finite values.
Results may differ from the reference program's by a relative error of at most 0.0042.
Values may be sent and summed in bfloat16 or wider, within the bound.
No kernel may reach another device: no remote copies, remote signals or barrier semaphores. Data moves between devices by JAX's collectives and lax.ppermute only.
A program may use at most 128 MiB of HBM per device.

```python
import math
import jax
import jax.numpy as jnp
import numpy as np
from jax import lax

NB = 98304
NOCC = 4096
SLAB_DEV = 8
BLK = 32
PTS = 128
BATCH = 128
LM = 49
SHELLS = 64
ATOM_DEV = 8
BLOCKS_DEV = 96
MOST = 14
NBLOCKS = 3072
SLAB = 256
POINTS = 4096
NBATCH = 32
ATOMS = 256
N_ROW = 4
N_COL = 8


def touch_ends(entries, key, low, top_value):
    longest = entries.shape.index(max(entries.shape))
    spots = []
    for shift in (0, 1):
        where = [jax.random.randint(jax.random.fold_in(key, axis), (), 0, length) for axis, length in enumerate(entries.shape)]
        where[longest] = (where[longest] + shift) % entries.shape[longest]
        spots.append(tuple(where))
    return entries.at[spots[0]].set(low).at[spots[1]].set(top_value)


def block_levels(rng, extent, cuts, low, largest):
    gain = 1.0
    for dim, parts in cuts:
        draws = jax.random.uniform(jax.random.fold_in(jax.random.fold_in(rng, 6), dim), (parts,), jnp.float32, low / len(cuts), largest / len(cuts))
        gain = gain * jnp.repeat(jnp.exp(draws), extent[dim] // parts).reshape((-1,) + (1,) * (len(extent) - 1 - dim))
    return gain


def routed_block(own_key, own, number, rows, number_of, top, limit, slope):
    order = jax.random.permutation(own_key, number_of)
    crowded, usual = load_shares(number_of, rows * top, limit, slope, True), load_shares(number_of, rows * top, limit, slope, False)
    places = jnp.arange(number_of)

    def named(sizes, offset_by):
        used = int((sizes > 0).sum())
        fixed = max(1, used // 4)
        shifted = fixed + (places - fixed + offset_by * (used - fixed)) % max(1, number_of - fixed)
        return jnp.zeros((number_of,), jnp.int32).at[order[jnp.where(places < fixed, places, shifted)]].set(jnp.asarray(sizes, jnp.int32))

    sizes = jnp.where(number % 4 == 0, named(crowded, number // 4), named(usual, number - number // 4 - 1))
    mixed = jax.random.permutation(jax.random.fold_in(own, 3), number_of)
    donor, receiver = mixed[0:number_of // 2 * 2:2], mixed[1:number_of // 2 * 2:2]
    margin = jnp.minimum(sizes[donor] - 1, limit - sizes[receiver]) // 2
    margin = jnp.where((donor == order[0]) | (receiver == order[0]) | (sizes[receiver] == 0), 0, jnp.maximum(margin, 0))
    shifted = jax.random.randint(jax.random.fold_in(own, 4), (number_of // 2,), 0, 1 << 20) % (margin + 1)
    sizes = sizes.at[donor].add(-shifted).at[receiver].add(shifted)
    items = jnp.searchsorted(jnp.cumsum(sizes), jnp.arange(rows * top), side="right").astype(jnp.int32)
    table = items.reshape(top, rows).T
    table = table[jax.random.permutation(jax.random.fold_in(own, 1), rows)]
    offset_by = jax.random.randint(jax.random.fold_in(own, 2), (rows, 1), 0, top)
    return jnp.take_along_axis(table, (jnp.arange(top)[None, :] + offset_by) % top, axis=1)


def load_shares(number_of, total, limit, lean, full):
    portions = [(1 << 20) // math.isqrt(grade ** lean) + 1 for grade in range(1, number_of + 1)]
    largest = limit if full else min(limit, max(-(-total // number_of), total * portions[0] // sum(portions)))
    least = 1 if total - largest >= number_of - 1 else 0
    counts, surplus = [largest] + [least] * (number_of - 1), total - largest - least * (number_of - 1)
    while surplus > 0:
        free = [i for i in range(1, number_of) if counts[i] < largest] or [i for i in range(1, number_of) if counts[i] < limit]
        pool, budget = sum([portions[i] for i in free]), surplus
        for i in free:
            more = min(limit - counts[i], max(1, budget * portions[i] // pool), surplus)
            counts[i] = counts[i] + more
            surplus = surplus - more
    return np.array(counts)


def bell_draw(rng, extent, width, limit, cuts=(), held_as=jnp.bfloat16):
    values = jax.random.normal(rng, extent, jnp.float32) * width
    if len(cuts) > 0:
        values = block_levels(rng, extent, cuts, -0.22, 0.18) * values
    return jnp.clip(values, min=-limit, max=limit).astype(held_as)


def setup_inputs(seed: int = 0) -> dict:
    splits = jax.random.split(jax.random.key(seed), 9)
    orbitals = bell_draw(splits[0], (NB, NOCC), NOCC ** -0.5, 0.09375, ((0, 32),))
    occupation = touch_ends(jax.random.randint(splits[1], (NOCC,), 1, 129), jax.random.fold_in(splits[1], 1), 1, 128).astype(jnp.int32)
    owner_keys = jax.random.split(jax.random.fold_in(splits[2], 1), NBLOCKS // BLOCKS_DEV)
    owner_turns = jax.random.permutation(jax.random.fold_in(splits[2], 3), NBLOCKS // BLOCKS_DEV)
    owner = jax.vmap(lambda own, number: routed_block(jax.random.fold_in(splits[2], 2), own, number, BLOCKS_DEV, N_COL, 1, MOST, 2))(owner_keys, owner_turns).reshape((NBLOCKS, 1))
    row_values = bell_draw(splits[3], (NB, PTS), 0.04, 0.23925781, ((0, 32),))
    slab_values = bell_draw(splits[4], (SLAB, POINTS), 1.0, 6.0, ((1, 32),))
    moment_weights = bell_draw(splits[5], (LM, POINTS), 0.1, 0.6, ((1, 32),), jnp.float32)
    batch_atom = touch_ends(jax.random.randint(splits[6], (NBATCH,), 0, ATOMS), jax.random.fold_in(splits[6], 1), 0, ATOMS - 1).astype(jnp.int32)
    batch_shell = touch_ends(jax.random.randint(splits[7], (NBATCH,), 0, SHELLS), jax.random.fold_in(splits[7], 1), 0, SHELLS - 1).astype(jnp.int32)
    return dict(orbitals=orbitals, occupation=occupation, owner=owner, row_values=row_values, slab_values=slab_values, moment_weights=moment_weights, batch_atom=batch_atom, batch_shell=batch_shell)


def reference(orbitals, occupation, owner, row_values, slab_values, moment_weights, batch_atom, batch_shell):
    devices = N_ROW * N_COL
    rows_dev = NB // devices
    nblocks = NB // BLK
    blocks_dev = rows_dev // BLK
    panel = orbitals.reshape(devices, rows_dev, NOCC)[:, :SLAB_DEV].reshape(devices * SLAB_DEV, NOCC)
    weights = occupation.astype(jnp.float32) / 64.0
    weighted = (panel.astype(jnp.float32) * weights[None, :]).astype(jnp.bfloat16)
    slab_matrix = lax.dot_general(orbitals, weighted, (((1,), (1,)), ((), ())), preferred_element_type=jnp.float32).astype(jnp.bfloat16)
    blocks = slab_matrix.reshape(nblocks, BLK, devices * SLAB_DEV)
    phis = row_values.reshape(nblocks, BLK, PTS)
    sender = jnp.arange(nblocks, dtype=jnp.int32) // blocks_dev
    target = ((sender // N_COL) * N_COL + owner[:, 0]).astype(jnp.int32)

    def one_block(index):
        dest = target[index]
        values = lax.dynamic_slice_in_dim(slab_values, (dest * PTS).astype(jnp.int32), PTS, 1)
        product = jnp.dot(blocks[index], values, preferred_element_type=jnp.float32)
        return jnp.sum(product * phis[index].astype(jnp.float32), axis=0)

    contributions = lax.map(one_block, jnp.arange(nblocks, dtype=jnp.int32))
    density = jax.ops.segment_sum(contributions, target, num_segments=devices).reshape(devices * PTS)
    nbatch = devices * PTS // BATCH
    shaped = moment_weights.reshape(LM, nbatch, BATCH)
    batch_moments = jnp.einsum('lbp,bp->bl', shaped, density.reshape(nbatch, BATCH), precision=lax.Precision.HIGHEST)
    bins = (batch_atom * SHELLS + batch_shell).astype(jnp.int32)
    natoms = ATOM_DEV * devices
    summed = jax.ops.segment_sum(batch_moments, bins, num_segments=natoms * SHELLS)
    moments = summed.T.reshape(LM, natoms, SHELLS)
    return density, moments
```

```python
import functools

import jax
import jax.numpy as jnp
from jax import lax
from jax.experimental import pallas as pl
from jax.experimental.pallas import tpu as pltpu
from jax.sharding import PartitionSpec as P

SLAB_DEV = 8
BLK = 32
BATCH = 128
SHELLS = 64
ATOM_DEV = 8
LMP = 64


def swap(x, axis, mask):
    size = lax.axis_size(axis)
    return lax.ppermute(x, axis, [(i, i ^ mask) for i in range(size)])


def masks_above(size, low):
    out = []
    m = size // 2
    while m >= low:
        out.append(m)
        m //= 2
    return out


def plan_kernel(ncol, most, own, pos, slot):
    my_col = pos[1]
    for t in range(ncol):
        slot[ncol * most + t] = t * most
    for s in range(ncol * most):
        slot[s] = -1

    def assign(b, c):
        at = ncol * most + (own[b] ^ my_col)
        s = slot[at]
        slot[at] = s + 1
        slot[s] = b
        return c

    lax.fori_loop(0, own.shape[0], assign, 0, unroll=4)


def plan(own, pos, ncol, most):
    smem = pl.BlockSpec(memory_space=pltpu.SMEM)
    return pl.pallas_call(
        functools.partial(plan_kernel, ncol, most),
        out_shape=jax.ShapeDtypeStruct((ncol * most + ncol,), jnp.int32),
        in_specs=[smem, smem],
        out_specs=smem,
        name="plan",
    )(own, pos)


def fold_kernel(most, first, slot, orb, phi, out, phit):
    def target(k, c):
        blocks = [slot[(first + k) * most + m] for m in range(most)]
        rows = [pl.ds(pl.multiple_of(jnp.maximum(b, 0) * BLK, BLK), BLK) for b in blocks]
        picked = []
        for b, at in zip(blocks, rows):
            block = phi[at]
            picked.append(jnp.where(b >= 0, block, jnp.zeros_like(block)))
        phit[...] = jnp.concatenate(picked, axis=0).T
        held = jnp.concatenate([orb[at] for at in rows], axis=0)
        acc = jnp.dot(phit[...], held, preferred_element_type=jnp.float32)
        out[k] = acc.astype(out.dtype)
        return c

    lax.fori_loop(0, out.shape[0], target, 0)


def fold(slot, orbitals, row_values, most, first, count):
    cols = orbitals.shape[1]
    points = row_values.shape[1]
    vmem = pl.BlockSpec(memory_space=pltpu.VMEM)
    smem = pl.BlockSpec(memory_space=pltpu.SMEM)
    return pl.pallas_call(
        functools.partial(fold_kernel, most, first),
        out_shape=jax.ShapeDtypeStruct((count, points, cols), jnp.bfloat16),
        in_specs=[smem, vmem, vmem],
        out_specs=vmem,
        scratch_shapes=[pltpu.VMEM((points, most * BLK), jnp.bfloat16)],
        compiler_params=pltpu.CompilerParams(vmem_limit_bytes=4 * 2**20),
        cost_estimate=pl.CostEstimate(
            flops=2 * count * most * BLK * cols * points,
            bytes_accessed=2 * count * most * BLK * cols,
            transcendentals=0,
        ),
        name="fold",
    )(slot, orbitals, row_values)


def body(
    orbitals, occupation, owner, row_values, slab_values, moment_weights, batch_atom, batch_shell
):
    nrow, ncol = lax.axis_size("row"), lax.axis_size("col")
    my_row, my_col = lax.axis_index("row"), lax.axis_index("col")
    pos = jnp.stack([my_row, my_col]).astype(jnp.int32)
    nblk = owner.shape[0]
    most = nblk // ncol + 2
    points = row_values.shape[1]
    lm = moment_weights.shape[0]
    cat = lambda xs: jnp.concatenate(xs, axis=0)

    weights = occupation.astype(jnp.float32) / 64.0
    mine = (orbitals[:SLAB_DEV].astype(jnp.float32) * weights[None, :]).astype(jnp.bfloat16)

    col_high = masks_above(ncol, 2)
    got, rel = [mine], [(0, 0)]
    for m in col_high:
        got = got + [swap(x, "col", m) for x in got]
        rel = rel + [(r, c ^ m) for r, c in rel]
    for m in masks_above(nrow, 4):
        got = got + [swap(x, "row", m) for x in got]
        rel = rel + [(r ^ m, c) for r, c in rel]
    base = cat(got)
    slot = plan(owner[:, 0], pos, ncol, most)
    early = ncol // 4
    table_a = fold(slot, orbitals, row_values, most, 0, early)
    table_b = fold(slot, orbitals, row_values, most, early, ncol - early)
    base, table_a = lax.optimization_barrier((base, table_a))
    across = swap(base, "row", 2)
    along = swap(base, "col", 1)
    half = base.shape[1] // 2
    diag_b = swap(along[:, half:], "row", 2)
    diag_a = swap(across[:, :half], "col", 1)
    far = lambda rm, cm, rl: [(r ^ rm, c ^ cm) for r, c in rl]
    n = base.shape[0]
    parts = []
    for k, (x, rl, col0) in enumerate(
        [
            (base, rel, 0),
            (across, far(2, 0, rel), 0),
            (along, far(0, 1, rel), 0),
            (diag_a, far(2, 1, rel), 0),
            (diag_b, far(2, 1, rel), half),
        ]
    ):
        row0 = min(k, 3) * n
        parts.append((x, row0, col0, rl))
        parts.append((swap(x, "row", 1), row0 + 4 * n, col0, far(1, 0, rl)))

    mw_hi = lax.reduce_precision(moment_weights, 8, 7)
    digits = [jnp.pad(x.astype(jnp.bfloat16), ((0, LMP - lm), (0, 0))) for x in (mw_hi, moment_weights - mw_hi)]
    local = cat([slab_values] + digits)
    vs, vrel = [cat([local, swap(local, "col", 1)])], [[0, 1]]
    for m in col_high:
        vs = vs + [swap(y, "col", m) for y in vs]
        vrel = vrel + [[c ^ m for c in r] for r in vrel]
    order = [c for r in vrel for c in r]

    own_bin = (batch_atom * SHELLS + batch_shell).astype(jnp.float32).reshape(1, 1)
    send = meet(parts, vs, order, [table_a, table_b], pos, own_bin, nrow, ncol)
    recv = lax.all_to_all(send, ("row", "col"), 0, 0, tiled=True)

    pm_rows = ncol // 2
    mine_rows = lax.dynamic_slice_in_dim(recv[:, pm_rows, :], my_row * ncol, ncol, 0)
    density = jnp.sum(mine_rows, axis=0)
    pm = jnp.sum(recv[:, :pm_rows, :].reshape(nrow, ncol, pm_rows, 2 * LMP), axis=1)
    pm = pm.reshape(nrow, pm_rows, 2, LMP).transpose(0, 2, 1, 3).reshape(nrow * ncol, LMP)
    bins = recv[:, pm_rows + 1, 0].astype(jnp.int32)
    start = (my_row * ncol + my_col) * (ATOM_DEV * SHELLS)
    local = jnp.arange(ATOM_DEV * SHELLS, dtype=jnp.int32) + start
    onehot = (bins[:, None] == local[None, :]).astype(jnp.float32)
    moments = jnp.dot(pm[:, :lm].T, onehot, precision=lax.Precision.HIGHEST)
    return density, moments.reshape(lm, ATOM_DEV, SHELLS)


def meet(parts, vs, order, tables, pos, own_bin, nrow, ncol):
    points, cols = tables[0].shape[1:]
    places = [(row0, col0) for _, row0, col0, _ in parts]
    pieces = [x for x, *_ in parts]
    slab = max(row0 + x.shape[0] for x, row0, *_ in parts)
    pm_rows = ncol // 2
    out_rows = -(-(pm_rows + 2) // 8) * 8
    pair = 2
    rel_of = {}
    for x, row0, _, rl in parts:
        for i, r in enumerate(rl):
            rel_of[row0 // SLAB_DEV + i] = r
    nv, nt = len(vs), len(tables)
    vrows = slab + 2 * LMP
    homes = [(i, k) for i, t in enumerate(tables) for k in range(0, t.shape[0], pair)]

    def kernel(pos_ref, bin_ref, *refs):
        piece_refs = refs[: len(pieces)]
        v_refs = refs[len(pieces) : len(pieces) + nv]
        c_refs = refs[len(pieces) + nv : len(pieces) + nv + nt]
        out, wt, vf, terms = refs[len(pieces) + nv + nt :]
        my_row, my_col = pos_ref[0], pos_ref[1]
        for ref, (row0, col0) in zip(piece_refs, places):
            wt[row0 : row0 + ref.shape[0], col0 : col0 + ref.shape[1]] = ref[...]
        where = {cm: (k // 2, (k % 2) * vrows) for k, cm in enumerate(order)}
        for cm, (a, base) in where.items():
            vf[cm] = v_refs[a][base : base + slab].astype(jnp.float32).reshape(slab // SLAB_DEV, SLAB_DEV, points)
        for g, (i, k) in enumerate(homes):
            two = lax.dot_general(
                wt[...],
                c_refs[i][k : k + pair].reshape(pair * points, cols),
                (((1,), (1,)), ((), ())),
                preferred_element_type=jnp.float32,
            )
            for q in range(pair):
                acc = jnp.zeros((SLAB_DEV, points), jnp.float32)
                for i, (rm, cm) in rel_of.items():
                    dev = (my_row ^ rm) * ncol + (my_col ^ cm)
                    acc += (
                        two[i * SLAB_DEV : (i + 1) * SLAB_DEV, q * points : (q + 1) * points]
                        * vf[g * pair + q, dev]
                    )
                terms[g * pair + q] = jnp.sum(acc, axis=0, keepdims=True)

        lhs_parts = []
        rhs_parts = []
        row_id = lax.broadcasted_iota(jnp.int32, (pm_rows, points), 0)
        for cm in range(ncol):
            t = my_col ^ cm
            a, base = where[cm]
            hi = v_refs[a][base + slab : base + slab + LMP].astype(jnp.float32)
            mw = hi + v_refs[a][base + slab + LMP : base + slab + 2 * LMP].astype(jnp.float32)
            lhs_parts.append(jnp.where(row_id == t % pm_rows, terms[cm], 0.0))
            low = t < pm_rows
            rhs_parts.append(jnp.concatenate([jnp.where(low, mw, 0.0), jnp.where(low, 0.0, mw)], axis=0))
        pm = lax.dot_general(
            jnp.concatenate(lhs_parts, axis=1),
            jnp.concatenate(rhs_parts, axis=1),
            (((1,), (1,)), ((), ())),
            precision=lax.Precision.HIGHEST,
            preferred_element_type=jnp.float32,
        )
        tail = jnp.full((1, points), bin_ref[0, 0], jnp.float32)
        fill = jnp.zeros((out_rows - pm_rows - 2, points), jnp.float32)
        for cm in range(ncol):
            t = my_col ^ cm
            block = jnp.concatenate([pm, terms[cm], tail, fill], axis=0)
            for r in range(nrow):
                out[r * ncol + t] = block

    vmem = pl.BlockSpec(memory_space=pltpu.VMEM)
    smem = pl.BlockSpec(memory_space=pltpu.SMEM)
    return pl.pallas_call(
        kernel,
        out_shape=jax.ShapeDtypeStruct((nrow * ncol, out_rows, points), jnp.float32),
        in_specs=[smem, smem] + [vmem] * (len(pieces) + nv + nt),
        out_specs=vmem,
        scratch_shapes=[
            pltpu.VMEM((slab, cols), jnp.bfloat16),
            pltpu.VMEM((ncol, slab // SLAB_DEV, SLAB_DEV, points), jnp.float32),
            pltpu.VMEM((ncol, 1, points), jnp.float32),
        ],
        compiler_params=pltpu.CompilerParams(vmem_limit_bytes=8 * 2**20 if slab <= 256 else 40 * 2**20),
        cost_estimate=pl.CostEstimate(
            flops=2 * slab * cols * ncol * points, bytes_accessed=2 * ncol * points * cols, transcendentals=0
        ),
        name="meet",
    )(pos, own_bin, *pieces, *vs, *tables)


def solution(mesh):
    placed = (
        P(("row", "col"), None),
        P(),
        P(("row", "col"), None),
        P(("row", "col"), None),
        P(None, ("row", "col")),
        P(None, ("row", "col")),
        P(("row", "col")),
        P(("row", "col")),
    )
    return jax.shard_map(
        body,
        mesh=mesh,
        in_specs=placed,
        out_specs=(P(("row", "col")), P(None, ("row", "col"), None)),
        check_vma=False,
    )
```

```python
import functools

import jax
import jax.numpy as jnp
from jax import lax
from jax.experimental import pallas as pl
from jax.experimental.pallas import tpu as pltpu
from jax.sharding import PartitionSpec as P


SLAB_DEV = 8
BLK = 32
SHELLS = 64
ATOM_DEV = 8
LMP = 64


def swap(x, axis, mask):
    size = lax.axis_size(axis)
    return lax.ppermute(x, axis, [(i, i ^ mask) for i in range(size)])


def round8(n):
    return -(-n // 8) * 8


def masks_above(size, low):
    out = []
    m = size // 2
    while m >= low:
        out.append(m)
        m //= 2
    return out


VMEM = pl.BlockSpec(memory_space=pltpu.VMEM)
SMEM = pl.BlockSpec(memory_space=pltpu.SMEM)


def weigh(orbitals, occupation):
    def kernel(rows, occ, out):
        weights = occ[...].astype(jnp.float32) / 64.0
        out[...] = (rows[...].astype(jnp.float32) * weights).astype(out.dtype)

    cols = orbitals.shape[1]
    return pl.pallas_call(
        kernel,
        out_shape=jax.ShapeDtypeStruct((SLAB_DEV, cols), jnp.bfloat16),
        in_specs=[VMEM, VMEM],
        out_specs=VMEM,
        compiler_params=pltpu.CompilerParams(vmem_limit_bytes=2**20),
        cost_estimate=pl.CostEstimate(flops=HINT_FLOPS, bytes_accessed=HINT_BYTES, transcendentals=0),
        name="weigh",
    )(orbitals[:SLAB_DEV], occupation.reshape(1, cols))


def plan_kernel(ncol, most, own, slot):
    my_col = lax.axis_index("col")
    for t in range(ncol):
        slot[ncol * most + t] = t * most
    for s in range(ncol * most):
        slot[s] = -1

    def assign(b, c):
        at = ncol * most + (own[b] ^ my_col)
        s = slot[at]
        slot[at] = s + 1
        slot[s] = b
        return c

    lax.fori_loop(0, own.shape[0], assign, 0, unroll=4)


def plan(own, ncol, most):
    return pl.pallas_call(
        functools.partial(plan_kernel, ncol, most),
        out_shape=jax.ShapeDtypeStruct((ncol * most + ncol,), jnp.int32),
        in_specs=[SMEM],
        out_specs=SMEM,
        compiler_params=pltpu.CompilerParams(vmem_limit_bytes=2**20),
        name="plan",
    )(own)


def pack_kernel(slab, mw, packed):
    rows, lm = slab.shape[0], mw.shape[0]
    high = mw[...].astype(jnp.bfloat16)
    low = (mw[...] - high.astype(jnp.float32)).astype(jnp.bfloat16)
    fill = jnp.zeros((round8(lm) - lm, mw.shape[1]), jnp.bfloat16)
    packed[:rows] = slab[...]
    packed[rows:] = jnp.concatenate([high, fill, low, fill], axis=0)


def pack(slab_values, moment_weights):
    rows, points = slab_values.shape
    return pl.pallas_call(
        pack_kernel,
        out_shape=jax.ShapeDtypeStruct((rows + 2 * round8(moment_weights.shape[0]), points), jnp.bfloat16),
        in_specs=[VMEM, VMEM],
        out_specs=VMEM,
        compiler_params=pltpu.CompilerParams(vmem_limit_bytes=2**20),
        name="pack",
    )(slab_values, moment_weights)


HINT_FLOPS = 10**10
HINT_BYTES = 3 * 10**7


def fold_kernel(most, first, slot, orb, phi, out, phit):
    def target(k, c):
        blocks = [slot[(first + k) * most + m] for m in range(most)]
        rows = [pl.ds(pl.multiple_of(jnp.maximum(b, 0) * BLK, BLK), BLK) for b in blocks]
        picked = []
        for b, at in zip(blocks, rows):
            block = phi[at]
            picked.append(jnp.where(b >= 0, block, jnp.zeros_like(block)))
        phit[...] = jnp.concatenate(picked, axis=0).T
        held = jnp.concatenate([orb[at] for at in rows], axis=0)
        acc = jnp.dot(phit[...], held, preferred_element_type=jnp.float32)
        out[k] = acc.astype(out.dtype)
        return c

    lax.fori_loop(0, out.shape[0], target, 0)


def fold(slot, orbitals, row_values, most, first, count):
    cols = orbitals.shape[1]
    points = row_values.shape[1]
    return pl.pallas_call(
        functools.partial(fold_kernel, most, first),
        out_shape=jax.ShapeDtypeStruct((count, points, cols), jnp.bfloat16),
        in_specs=[SMEM, VMEM, VMEM],
        out_specs=VMEM,
        scratch_shapes=[pltpu.VMEM((points, most * BLK), jnp.bfloat16)],
        compiler_params=pltpu.CompilerParams(vmem_limit_bytes=4 * 2**20),
        cost_estimate=pl.CostEstimate(
            flops=2 * count * most * BLK * cols * points,
            bytes_accessed=2 * count * most * BLK * cols,
            transcendentals=0,
        ),
    )(slot, orbitals, row_values)


def body(
    orbitals, occupation, owner, row_values, slab_values, moment_weights, batch_atom, batch_shell
):
    nrow, ncol = lax.axis_size("row"), lax.axis_size("col")
    nblk = owner.shape[0]
    most = nblk // ncol + 2
    lm = moment_weights.shape[0]
    cat = lambda xs: jnp.concatenate(xs, axis=0)
    far = lambda rm, cm, rl: [(r ^ rm, c ^ cm) for r, c in rl]

    mine = weigh(orbitals, occupation)
    local = pack(slab_values, moment_weights)
    slot = plan(owner[:, 0], ncol, most)
    early = ncol // 4
    tables = [
        fold(slot, orbitals, row_values, most, 0, early), fold(slot, orbitals, row_values, most, early, ncol - early)
    ]

    col_high = masks_above(ncol, 2)
    got, rel = [mine], [(0, 0)]
    for m in col_high:
        got = got + [swap(x, "col", m) for x in got]
        rel = rel + far(0, m, rel)
    for m in masks_above(nrow, 4):
        got = got + [swap(x, "row", m) for x in got]
        rel = rel + far(m, 0, rel)
    base = cat(got)
    across = swap(base, "row", 2)
    along = swap(base, "col", 1)
    diag = swap(along, "row", 2)
    n = base.shape[0]
    parts = []
    for k, (x, rl, col0) in enumerate(
        [
            (base, rel, 0),
            (across, far(2, 0, rel), 0),
            (along, far(0, 1, rel), 0),
            (diag, far(2, 1, rel), 0),
        ]
    ):
        row0 = min(k, 3) * n
        parts.append((x, row0, col0, rl))
        parts.append((swap(x, "row", 1), row0 + 4 * n, col0, far(1, 0, rl)))

    vs = [(local, 0)]
    for m in col_high:
        vs = vs + [(swap(y, "col", m), c ^ m) for y, c in vs]
    near = []
    rest = list(vs)
    vs, order = [], []
    for group in (near, rest):
        if group:
            both = cat([y for y, _ in group])
            cms = [c for _, c in group]
            vs += [both, swap(both, "col", 1)]
            order += [cms, [c ^ 1 for c in cms]]

    send = meet(parts, vs, order, tables, batch_atom.reshape(1, 1), batch_shell.reshape(1, 1), nrow, ncol)
    recv = lax.all_to_all(send, ("row", "col"), 0, 0, tiled=True)
    start = (lax.axis_index("row") * ncol + lax.axis_index("col")) * (ATOM_DEV * SHELLS)
    bins = jnp.arange(ATOM_DEV * SHELLS, dtype=jnp.int32).reshape(1, -1) + start
    density, moments = gather_up(recv, bins, lm, nrow, ncol)
    return density.reshape(-1), moments


def gather_up(recv, bins, lm, nrow, ncol):
    points = recv.shape[2]
    pm_rows = ncol // 2

    def kernel(got, bins, density, moments):
        my_row = lax.axis_index("row")
        total = got[my_row * ncol]
        for c in range(1, ncol):
            total = total + got[my_row * ncol + c]
        density[...] = total[pm_rows : pm_rows + 1]
        left, right = [], []
        for r in range(nrow):
            acc = got[r * ncol, :pm_rows]
            for c in range(1, ncol):
                acc = acc + got[r * ncol + c, :pm_rows]
            left.append(acc[:, :LMP])
            right.append(acc[:, LMP:])
        low = cat0([got[r * ncol + t, pm_rows + 1 : pm_rows + 2] for r in range(nrow) for t in range(pm_rows)])
        high = cat0(
            [got[r * ncol + pm_rows + t, pm_rows + 1 : pm_rows + 2] for r in range(nrow) for t in range(pm_rows)]
        )
        pm = cat0(left + right)
        bin_of = cat0([low, high]).astype(jnp.int32)
        width = bin_of.shape[1]
        hot = jnp.concatenate(
            [
                (bin_of == bins[:, k : k + width]).astype(jnp.float32)
                for k in range(0, bins.shape[1], width)
            ],
            axis=1,
        )
        placed = lax.dot_general(
            pm,
            hot,
            (((0,), (0,)), ((), ())),
            precision=lax.Precision.HIGHEST,
            preferred_element_type=jnp.float32,
        )
        for a in range(ATOM_DEV):
            moments[:, a, :] = placed[:lm, a * SHELLS : (a + 1) * SHELLS]

    return pl.pallas_call(
        kernel,
        out_shape=[
            jax.ShapeDtypeStruct((1, points), jnp.float32),
            jax.ShapeDtypeStruct((lm, ATOM_DEV, SHELLS), jnp.float32),
        ],
        in_specs=[VMEM, VMEM],
        out_specs=[VMEM, VMEM],
        compiler_params=pltpu.CompilerParams(vmem_limit_bytes=4 * 2**20),
        name="gather_up",
    )(recv, bins)


def cat0(xs):
    return jnp.concatenate(xs, axis=0)


def meet(parts, vs, order, tables, atom, shell, nrow, ncol):
    points, cols = tables[0].shape[1:]
    early = tables[0].shape[0]
    places = [(row0, col0) for _, row0, col0, _ in parts]
    pieces = [x for x, *_ in parts]
    slab = max(row0 + x.shape[0] for x, row0, *_ in parts)
    pm_rows = ncol // 2
    out_rows = round8(pm_rows + 2)
    pair = 2
    rel_of = {}
    for x, row0, _, rl in parts:
        for i, r in enumerate(rl):
            rel_of[row0 // SLAB_DEV + i] = r
    part = (vs[0].shape[0] // len(order[0]) - slab) // 2
    vrows = slab + 2 * part
    nv = len(vs)

    def kernel(*refs):
        piece_refs = refs[: len(pieces)]
        v_refs = refs[len(pieces) : len(pieces) + nv]
        atom_ref, shell_ref, c_low, c_high, out, wt, vf, terms = refs[len(pieces) + nv :]
        where = {cm: (v_refs[a], k * vrows) for a, cms in enumerate(order) for k, cm in enumerate(cms)}
        my_row, my_col = lax.axis_index("row"), lax.axis_index("col")
        for ref, (row0, col0) in zip(piece_refs, places):
            wt[row0 : row0 + ref.shape[0], col0 : col0 + ref.shape[1]] = ref[...]
        for cm in range(ncol):
            ref, at = where[cm]
            vf[cm] = ref[at : at + slab].astype(jnp.float32).reshape(slab // SLAB_DEV, SLAB_DEV, points)

        def targets(c_ref, at, first, many):
            two = lax.dot_general(
                wt[...],
                c_ref[pl.ds(at, many)].reshape(many * points, cols),
                (((1,), (1,)), ((), ())),
                preferred_element_type=jnp.float32,
            )
            for q in range(many):
                acc = jnp.zeros((SLAB_DEV, points), jnp.float32)
                for i, (rm, cm) in rel_of.items():
                    dev = (my_row ^ rm) * ncol + (my_col ^ cm)
                    acc += (
                        two[i * SLAB_DEV : (i + 1) * SLAB_DEV, q * points : (q + 1) * points]
                        * vf[first + q, dev]
                    )
                terms[first + q] = jnp.sum(acc, axis=0, keepdims=True)

        for c_ref, base in ((c_low, 0), (c_high, early)):
            count = c_ref.shape[0]
            if ncol <= 8:
                for at in range(0, count, pair):
                    targets(c_ref, at, base + at, min(pair, count - at))
            else:

                def both(g, c, c_ref=c_ref, base=base):
                    targets(c_ref, g * pair, base + g * pair, pair)
                    return c

                lax.fori_loop(0, count // pair, both, 0)

        lhs_parts = []
        rhs_parts = []
        row_id = lax.broadcasted_iota(jnp.int32, (pm_rows, points), 0)
        for cm in range(ncol):
            t = my_col ^ cm
            ref, at = where[cm]
            mw = ref[at + slab : at + slab + part].astype(jnp.float32)
            mw = mw + ref[at + slab + part : at + vrows].astype(jnp.float32)
            mw = jnp.concatenate([mw, jnp.zeros((LMP - part, points), jnp.float32)], axis=0)
            lhs_parts.append(jnp.where(row_id == t % pm_rows, terms[cm], 0.0))
            low = t < pm_rows
            rhs_parts.append(jnp.concatenate([jnp.where(low, mw, 0.0), jnp.where(low, 0.0, mw)], axis=0))
        pm = lax.dot_general(
            jnp.concatenate(lhs_parts, axis=1),
            jnp.concatenate(rhs_parts, axis=1),
            (((1,), (1,)), ((), ())),
            precision=lax.Precision.HIGHEST,
            preferred_element_type=jnp.float32,
        )
        own_bin = (atom_ref[...] * SHELLS + shell_ref[...]).astype(jnp.float32)
        tail = jnp.broadcast_to(own_bin, (1, points))
        fill = jnp.zeros((out_rows - pm_rows - 2, points), jnp.float32)
        for cm in range(ncol):
            t = my_col ^ cm
            block = jnp.concatenate([pm, terms[cm], tail, fill], axis=0)
            for r in range(nrow):
                out[r * ncol + t] = block

    return pl.pallas_call(
        kernel,
        out_shape=jax.ShapeDtypeStruct((nrow * ncol, out_rows, points), jnp.float32),
        in_specs=[VMEM] * (len(pieces) + nv + 4),
        out_specs=VMEM,
        scratch_shapes=[
            pltpu.VMEM((slab, cols), jnp.bfloat16),
            pltpu.VMEM((ncol, slab // SLAB_DEV, SLAB_DEV, points), jnp.float32),
            pltpu.VMEM((ncol, 1, points), jnp.float32),
        ],
        compiler_params=pltpu.CompilerParams(vmem_limit_bytes=8 * 2**20 if slab <= 256 else 40 * 2**20),
        cost_estimate=pl.CostEstimate(
            flops=2 * slab * cols * ncol * points, bytes_accessed=2 * ncol * points * cols, transcendentals=0
        ),
        name="meet",
    )(*pieces, *vs, atom, shell, *tables)


def solution(mesh):
    placed = (
        P(("row", "col"), None),
        P(),
        P(("row", "col"), None),
        P(("row", "col"), None),
        P(None, ("row", "col")),
        P(None, ("row", "col")),
        P(("row", "col")),
        P(("row", "col")),
    )
    return jax.shard_map(
        body,
        mesh=mesh,
        in_specs=placed,
        out_specs=(P(("row", "col")), P(None, ("row", "col"), None)),
        check_vma=False,
    )
```

```python
import functools

import jax
import jax.numpy as jnp
from jax import lax
from jax.experimental import pallas as pl
from jax.experimental.pallas import tpu as pltpu
from jax.sharding import PartitionSpec as P


SLAB_DEV = 8
BLK = 32
SHELLS = 64
ATOM_DEV = 8
LMP = 64


def swap(x, axis, mask):
    size = lax.axis_size(axis)
    return lax.ppermute(x, axis, [(i, i ^ mask) for i in range(size)])


def round8(n):
    return -(-n // 8) * 8


def masks_above(size, low):
    out = []
    m = size // 2
    while m >= low:
        out.append(m)
        m //= 2
    return out


VMEM = pl.BlockSpec(memory_space=pltpu.VMEM)
SMEM = pl.BlockSpec(memory_space=pltpu.SMEM)


def weigh(orbitals, occupation):
    def kernel(rows, occ, out):
        weights = occ[...].astype(jnp.float32) / 64.0
        out[...] = (rows[...].astype(jnp.float32) * weights).astype(out.dtype)

    cols = orbitals.shape[1]
    return pl.pallas_call(
        kernel,
        out_shape=jax.ShapeDtypeStruct((SLAB_DEV, cols), jnp.bfloat16),
        in_specs=[VMEM, VMEM],
        out_specs=VMEM,
        compiler_params=pltpu.CompilerParams(vmem_limit_bytes=2**20),
        cost_estimate=pl.CostEstimate(flops=HINT_FLOPS, bytes_accessed=HINT_BYTES, transcendentals=0),
        name="weigh",
    )(orbitals[:SLAB_DEV], occupation.reshape(1, cols))


def plan_kernel(ncol, most, own, slot):
    my_col = lax.axis_index("col")
    for t in range(ncol):
        slot[ncol * most + t] = t * most
    for s in range(ncol * most):
        slot[s] = -1

    def assign(b, c):
        at = ncol * most + (own[b] ^ my_col)
        s = slot[at]
        slot[at] = s + 1
        slot[s] = b
        return c

    lax.fori_loop(0, own.shape[0], assign, 0, unroll=4)


def plan(own, ncol, most):
    return pl.pallas_call(
        functools.partial(plan_kernel, ncol, most),
        out_shape=jax.ShapeDtypeStruct((ncol * most + ncol,), jnp.int32),
        in_specs=[SMEM],
        out_specs=SMEM,
        compiler_params=pltpu.CompilerParams(vmem_limit_bytes=2**20),
        name="plan",
    )(own)


def pack_kernel(slab, mw, packed):
    rows, lm = slab.shape[0], mw.shape[0]
    high = mw[...].astype(jnp.bfloat16)
    low = (mw[...] - high.astype(jnp.float32)).astype(jnp.bfloat16)
    fill = jnp.zeros((round8(lm) - lm, mw.shape[1]), jnp.bfloat16)
    packed[:rows] = slab[...]
    packed[rows:] = jnp.concatenate([high, fill, low, fill], axis=0)


def pack(slab_values, moment_weights):
    rows, points = slab_values.shape
    return pl.pallas_call(
        pack_kernel,
        out_shape=jax.ShapeDtypeStruct((rows + 2 * round8(moment_weights.shape[0]), points), jnp.bfloat16),
        in_specs=[VMEM, VMEM],
        out_specs=VMEM,
        compiler_params=pltpu.CompilerParams(vmem_limit_bytes=2**20),
        name="pack",
    )(slab_values, moment_weights)


HINT_FLOPS = 10**10
HINT_BYTES = 3 * 10**7


def fold_kernel(most, first, slot, orb, phi, out, phit):
    def target(k, c):
        blocks = [slot[(first + k) * most + m] for m in range(most)]
        rows = [pl.ds(pl.multiple_of(jnp.maximum(b, 0) * BLK, BLK), BLK) for b in blocks]
        picked = []
        for b, at in zip(blocks, rows):
            block = phi[at]
            picked.append(jnp.where(b >= 0, block, jnp.zeros_like(block)))
        phit[...] = jnp.concatenate(picked, axis=0).T
        held = jnp.concatenate([orb[at] for at in rows], axis=0)
        acc = jnp.dot(phit[...], held, preferred_element_type=jnp.float32)
        out[k] = acc.astype(out.dtype)
        return c

    lax.fori_loop(0, out.shape[0], target, 0)


def fold(slot, orbitals, row_values, most, first, count):
    cols = orbitals.shape[1]
    points = row_values.shape[1]
    return pl.pallas_call(
        functools.partial(fold_kernel, most, first),
        out_shape=jax.ShapeDtypeStruct((count, points, cols), jnp.bfloat16),
        in_specs=[SMEM, VMEM, VMEM],
        out_specs=VMEM,
        scratch_shapes=[pltpu.VMEM((points, most * BLK), jnp.bfloat16)],
        compiler_params=pltpu.CompilerParams(vmem_limit_bytes=4 * 2**20),
        cost_estimate=pl.CostEstimate(
            flops=2 * count * most * BLK * cols * points,
            bytes_accessed=2 * count * most * BLK * cols,
            transcendentals=0,
        ),
    )(slot, orbitals, row_values)


def body(
    orbitals, occupation, owner, row_values, slab_values, moment_weights, batch_atom, batch_shell
):
    nrow, ncol = lax.axis_size("row"), lax.axis_size("col")
    nblk = owner.shape[0]
    most = nblk // ncol + 2
    lm = moment_weights.shape[0]
    cat = lambda xs: jnp.concatenate(xs, axis=0)
    far = lambda rm, cm, rl: [(r ^ rm, c ^ cm) for r, c in rl]

    mine = weigh(orbitals, occupation)
    local = pack(slab_values, moment_weights)
    slot = plan(owner[:, 0], ncol, most)
    early = ncol // 4
    tables = [
        fold(slot, orbitals, row_values, most, 0, early), fold(slot, orbitals, row_values, most, early, ncol - early)
    ]

    col_high = masks_above(ncol, 2)
    got, rel = [mine], [(0, 0)]
    for m in col_high:
        got = got + [swap(x, "col", m) for x in got]
        rel = rel + far(0, m, rel)
    for m in masks_above(nrow, 4):
        got = got + [swap(x, "row", m) for x in got]
        rel = rel + far(m, 0, rel)
    own_y = swap(mine, "col", 1)
    base = cat(got)
    others = cat(got[1:])
    across = swap(base, "row", 2)
    along = swap(others, "col", 1)
    first = cat([own_y, swap(own_y, "row", 2)])
    diag = swap(along, "row", 2)
    parts, row0 = [], 0
    for x, rl in [
        (base, rel),
        (across, far(2, 0, rel)),
        (first, [(0, 1), (2, 1)]),
        (along, far(0, 1, rel[1:])),
        (diag, far(2, 1, rel[1:])),
    ]:
        n = x.shape[0]
        parts.append((x, row0, 0, rl))
        parts.append((swap(x, "row", 1), row0 + n, 0, far(1, 0, rl)))
        row0 += 2 * n

    vs = [(local, 0)]
    for m in col_high:
        vs = vs + [(swap(y, "col", m), c ^ m) for y, c in vs]
    near = []
    rest = list(vs)
    vs, order = [], []
    for group in (near, rest):
        if group:
            both = cat([y for y, _ in group])
            cms = [c for _, c in group]
            vs += [both, swap(both, "col", 1)]
            order += [cms, [c ^ 1 for c in cms]]

    send = meet(parts, vs, order, tables, batch_atom.reshape(1, 1), batch_shell.reshape(1, 1), nrow, ncol)
    recv = lax.all_to_all(send, ("row", "col"), 0, 0, tiled=True)
    start = (lax.axis_index("row") * ncol + lax.axis_index("col")) * (ATOM_DEV * SHELLS)
    bins = jnp.arange(ATOM_DEV * SHELLS, dtype=jnp.int32).reshape(1, -1) + start
    density, moments = gather_up(recv, bins, lm, nrow, ncol)
    return density.reshape(-1), moments


def gather_up(recv, bins, lm, nrow, ncol):
    points = recv.shape[2]
    pm_rows = ncol // 2

    def kernel(got, bins, density, moments):
        my_row = lax.axis_index("row")
        total = got[my_row * ncol]
        for c in range(1, ncol):
            total = total + got[my_row * ncol + c]
        density[...] = total[pm_rows : pm_rows + 1]
        left, right = [], []
        for r in range(nrow):
            acc = got[r * ncol, :pm_rows]
            for c in range(1, ncol):
                acc = acc + got[r * ncol + c, :pm_rows]
            left.append(acc[:, :LMP])
            right.append(acc[:, LMP:])
        low = cat0([got[r * ncol + t, pm_rows + 1 : pm_rows + 2] for r in range(nrow) for t in range(pm_rows)])
        high = cat0(
            [got[r * ncol + pm_rows + t, pm_rows + 1 : pm_rows + 2] for r in range(nrow) for t in range(pm_rows)]
        )
        pm = cat0(left + right)
        bin_of = cat0([low, high]).astype(jnp.int32)
        width = bin_of.shape[1]
        hot = jnp.concatenate(
            [
                (bin_of == bins[:, k : k + width]).astype(jnp.float32)
                for k in range(0, bins.shape[1], width)
            ],
            axis=1,
        )
        placed = lax.dot_general(
            pm,
            hot,
            (((0,), (0,)), ((), ())),
            precision=lax.Precision.HIGHEST,
            preferred_element_type=jnp.float32,
        )
        for a in range(ATOM_DEV):
            moments[:, a, :] = placed[:lm, a * SHELLS : (a + 1) * SHELLS]

    return pl.pallas_call(
        kernel,
        out_shape=[
            jax.ShapeDtypeStruct((1, points), jnp.float32),
            jax.ShapeDtypeStruct((lm, ATOM_DEV, SHELLS), jnp.float32),
        ],
        in_specs=[VMEM, VMEM],
        out_specs=[VMEM, VMEM],
        compiler_params=pltpu.CompilerParams(vmem_limit_bytes=4 * 2**20),
        name="gather_up",
    )(recv, bins)


def cat0(xs):
    return jnp.concatenate(xs, axis=0)


def meet(parts, vs, order, tables, atom, shell, nrow, ncol):
    points, cols = tables[0].shape[1:]
    early = tables[0].shape[0]
    places = [(row0, col0) for _, row0, col0, _ in parts]
    pieces = [x for x, *_ in parts]
    slab = max(row0 + x.shape[0] for x, row0, *_ in parts)
    pm_rows = ncol // 2
    out_rows = round8(pm_rows + 2)
    pair = 2
    rel_of = {}
    for x, row0, _, rl in parts:
        for i, r in enumerate(rl):
            rel_of[row0 // SLAB_DEV + i] = r
    part = (vs[0].shape[0] // len(order[0]) - slab) // 2
    vrows = slab + 2 * part
    nv = len(vs)

    def kernel(*refs):
        piece_refs = refs[: len(pieces)]
        v_refs = refs[len(pieces) : len(pieces) + nv]
        atom_ref, shell_ref, c_low, c_high, out, wt, vf, terms = refs[len(pieces) + nv :]
        where = {cm: (v_refs[a], k * vrows) for a, cms in enumerate(order) for k, cm in enumerate(cms)}
        my_row, my_col = lax.axis_index("row"), lax.axis_index("col")
        for ref, (row0, col0) in zip(piece_refs, places):
            wt[row0 : row0 + ref.shape[0], col0 : col0 + ref.shape[1]] = ref[...]
        for cm in range(ncol):
            ref, at = where[cm]
            vf[cm] = ref[at : at + slab].astype(jnp.float32).reshape(slab // SLAB_DEV, SLAB_DEV, points)

        def targets(c_ref, at, first, many):
            two = lax.dot_general(
                wt[...],
                c_ref[pl.ds(at, many)].reshape(many * points, cols),
                (((1,), (1,)), ((), ())),
                preferred_element_type=jnp.float32,
            )
            for q in range(many):
                acc = jnp.zeros((SLAB_DEV, points), jnp.float32)
                for i, (rm, cm) in rel_of.items():
                    dev = (my_row ^ rm) * ncol + (my_col ^ cm)
                    acc += (
                        two[i * SLAB_DEV : (i + 1) * SLAB_DEV, q * points : (q + 1) * points]
                        * vf[first + q, dev]
                    )
                terms[first + q] = jnp.sum(acc, axis=0, keepdims=True)

        for c_ref, base in ((c_low, 0), (c_high, early)):
            count = c_ref.shape[0]
            if ncol <= 8:
                for at in range(0, count, pair):
                    targets(c_ref, at, base + at, min(pair, count - at))
            else:

                def both(g, c, c_ref=c_ref, base=base):
                    targets(c_ref, g * pair, base + g * pair, pair)
                    return c

                lax.fori_loop(0, count // pair, both, 0)

        lhs_parts = []
        rhs_parts = []
        row_id = lax.broadcasted_iota(jnp.int32, (pm_rows, points), 0)
        for cm in range(ncol):
            t = my_col ^ cm
            ref, at = where[cm]
            mw = ref[at + slab : at + slab + part].astype(jnp.float32)
            mw = mw + ref[at + slab + part : at + vrows].astype(jnp.float32)
            mw = jnp.concatenate([mw, jnp.zeros((LMP - part, points), jnp.float32)], axis=0)
            lhs_parts.append(jnp.where(row_id == t % pm_rows, terms[cm], 0.0))
            low = t < pm_rows
            rhs_parts.append(jnp.concatenate([jnp.where(low, mw, 0.0), jnp.where(low, 0.0, mw)], axis=0))
        pm = lax.dot_general(
            jnp.concatenate(lhs_parts, axis=1),
            jnp.concatenate(rhs_parts, axis=1),
            (((1,), (1,)), ((), ())),
            precision=lax.Precision.HIGHEST,
            preferred_element_type=jnp.float32,
        )
        own_bin = (atom_ref[...] * SHELLS + shell_ref[...]).astype(jnp.float32)
        tail = jnp.broadcast_to(own_bin, (1, points))
        fill = jnp.zeros((out_rows - pm_rows - 2, points), jnp.float32)
        for cm in range(ncol):
            t = my_col ^ cm
            block = jnp.concatenate([pm, terms[cm], tail, fill], axis=0)
            for r in range(nrow):
                out[r * ncol + t] = block

    return pl.pallas_call(
        kernel,
        out_shape=jax.ShapeDtypeStruct((nrow * ncol, out_rows, points), jnp.float32),
        in_specs=[VMEM] * (len(pieces) + nv + 4),
        out_specs=VMEM,
        scratch_shapes=[
            pltpu.VMEM((slab, cols), jnp.bfloat16),
            pltpu.VMEM((ncol, slab // SLAB_DEV, SLAB_DEV, points), jnp.float32),
            pltpu.VMEM((ncol, 1, points), jnp.float32),
        ],
        compiler_params=pltpu.CompilerParams(vmem_limit_bytes=8 * 2**20 if slab <= 256 else 40 * 2**20),
        cost_estimate=pl.CostEstimate(
            flops=2 * slab * cols * ncol * points, bytes_accessed=2 * ncol * points * cols, transcendentals=0
        ),
        name="meet",
    )(*pieces, *vs, atom, shell, *tables)


def solution(mesh):
    placed = (
        P(("row", "col"), None),
        P(),
        P(("row", "col"), None),
        P(("row", "col"), None),
        P(None, ("row", "col")),
        P(None, ("row", "col")),
        P(("row", "col")),
        P(("row", "col")),
    )
    return jax.shard_map(
        body,
        mesh=mesh,
        in_specs=placed,
        out_specs=(P(("row", "col")), P(None, ("row", "col"), None)),
        check_vma=False,
    )
```
